32 devices in a mesh: mpo: 4 (over y, x), sec: 8 (over z, core).
Axes of the slice: x: 2, y: 2, z: 4, core: 2. Of those that a mesh axis runs over, the one named last changes fastest.
Arguments:
- wavefunction: bfloat16 [8, 256, 256], P('sec'), may hold values from -6 to 6
- left_dims: int32 [8], P('sec'), may hold values from 64 to 256
- right_dims: int32 [8], P('sec'), may hold values from 64 to 256
- left_environment_block: bfloat16 [1280, 256, 256], P(('mpo', 'sec')), may hold values from -0.375 to 0.375
- right_env: bfloat16 [1280, 256, 256], P(('mpo', 'sec')), may hold values from -0.03125 to 0.03125
- task_out: int32 [1280], P(('mpo', 'sec')), may hold values from 0 to 7
- task_in: int32 [1280], P(('mpo', 'sec')), may hold values from 0 to 7
Outputs:
- applied: bfloat16 [8, 256, 256], P('sec', 'mpo')
The draws below stay inside these ranges and needn't reach their ends.
All inputs are finite; a program needn't handle non-finite values.
Results may differ from the reference program's by a relative error of at most 0.0078.
Values may be sent and summed in bfloat16 or wider, within the bound.
A program may use at most 128 MiB of HBM per device.

```python
import math
import jax
import jax.numpy as jnp
import numpy as np
from jax import lax

BLK = 256
TASKS_DEV = 40
S = 8
TASKS = 1280


def place_ends(array, own_key, least, high):
    longest = array.shape.index(max(array.shape))
    spots = []
    for shift in (0, 1):
        where = [jax.random.randint(jax.random.fold_in(own_key, axis), (), 0, length) for axis, length in enumerate(array.shape)]
        where[longest] = (where[longest] + shift) % array.shape[longest]
        spots.append(tuple(where))
    return array.at[spots[0]].set(least).at[spots[1]].set(high)


def levels(stream_key, extent, split, low, high):
    level, own = 1.0, jax.random.fold_in(stream_key, 6)
    for dim, blocks in split:
        draws = jnp.exp(jax.random.uniform(jax.random.fold_in(own, dim), (blocks,), jnp.float32, low / len(split), high / len(split)))
        level = level * jnp.repeat(draws, extent[dim] // blocks).reshape([-1 if axis == dim else 1 for axis in range(len(extent))])
    return level


def cumulative_ranks(count, lean):
    weights = [(1 << 20) // math.isqrt(grade ** lean) + 1 for grade in range(1, count + 1)]
    width = 1 + sum(weights) // (1 << 30)
    return np.cumsum(np.array([max(1, weight // width) for weight in weights]))


def skewed_ids(own_key, dims, number_of, skew):
    table = cumulative_ranks(number_of, skew)
    ticket = jax.random.randint(jax.random.fold_in(own_key, 1), dims, 0, int(table[number_of - 1]))
    grade = jnp.searchsorted(jnp.asarray(table, jnp.int32), ticket, side="right")
    return jax.random.permutation(jax.random.fold_in(own_key, 2), number_of)[grade].astype(jnp.int32)


def scatter_about(stream_key, shape, deviation, limit, cuts=(), dtype=jnp.bfloat16):
    factor_of = levels(stream_key, shape, cuts, -0.22, 0.18) if cuts else 1.0
    drawn = jax.random.normal(stream_key, shape, jnp.float32) * deviation * factor_of
    return jnp.minimum(jnp.maximum(drawn, -limit), limit).astype(dtype)


def setup_inputs(seed: int = 0) -> dict:
    splits = jax.random.split(jax.random.key(seed), 8)
    return {
        "wavefunction": scatter_about(splits[0], (S, BLK, BLK), 1.0, 6.0, ((0, 8),)),
        "left_dims": place_ends(jax.random.randint(splits[1], (S,), BLK // 4, BLK + 1), jax.random.fold_in(splits[1], 1), BLK // 4, BLK).astype(jnp.int32),
        "right_dims": place_ends(jax.random.randint(splits[2], (S,), BLK // 4, BLK + 1), jax.random.fold_in(splits[2], 1), BLK // 4, BLK).astype(jnp.int32),
        "left_environment_block": scatter_about(splits[3], (TASKS, BLK, BLK), BLK ** -0.5, 0.375, ((0, 32),)),
        "right_env": scatter_about(splits[4], (TASKS, BLK, BLK), (BLK * TASKS // S) ** -0.5, 0.03125, ((0, 32),)),
        "task_out": place_ends(skewed_ids(splits[5], (TASKS,), S, 1), jax.random.fold_in(splits[5], 3), 0, S - 1).astype(jnp.int32),
        "task_in": place_ends(jax.random.randint(splits[6], (TASKS,), 0, S), jax.random.fold_in(splits[6], 1), 0, S - 1).astype(jnp.int32),
    }


def reference(wavefunction, left_dims, right_dims, left_environment_block, right_env, task_out, task_in):
    row_ids = lax.broadcasted_iota(jnp.int32, wavefunction.shape, 1)
    col_ids = lax.broadcasted_iota(jnp.int32, wavefunction.shape, 2)
    live_cells = (row_ids < left_dims[:, None, None]) & (col_ids < right_dims[:, None, None])
    masked = jnp.where(live_cells, wavefunction, jnp.zeros_like(wavefunction))
    rounds = TASKS // TASKS_DEV
    left_parts = left_environment_block.reshape(rounds, TASKS_DEV, BLK, BLK)
    right_parts = right_env.reshape(rounds, TASKS_DEV, BLK, BLK)
    out_parts = task_out.astype(jnp.int32).reshape(rounds, TASKS_DEV)
    input_pieces = task_in.astype(jnp.int32).reshape(rounds, TASKS_DEV)

    def accumulate(summed, pieces):
        left_piece, right_piece, out_ids, in_ids = pieces
        picked_tasks = jnp.take(masked, in_ids, axis=0).astype(jnp.float32)
        middle_tensor = jnp.einsum("xvz,xzy->xvy", left_piece.astype(jnp.float32), picked_tasks).astype(jnp.bfloat16)
        task_product = jnp.einsum("hzk,hlk->hzl", middle_tensor.astype(jnp.float32), right_piece.astype(jnp.float32))
        return summed + jax.ops.segment_sum(task_product, out_ids, num_segments=S), None

    summed, _ = lax.scan(accumulate, jnp.zeros((S, BLK, BLK), jnp.float32), (left_parts, right_parts, out_parts, input_pieces))
    return jnp.where(live_cells, summed, jnp.zeros_like(summed)).astype(jnp.bfloat16)
```

```python
import functools

import jax
import jax.numpy as jnp
from jax import lax
from jax.experimental import pallas as pl
from jax.experimental.pallas import tpu as pltpu
from jax.sharding import PartitionSpec as P

CORES = 2
GROUP = 4


def live(shape, row0, rows, cols):
    row_ids = lax.broadcasted_iota(jnp.int32, shape, 0) + row0
    col_ids = lax.broadcasted_iota(jnp.int32, shape, 1)
    return (row_ids < rows) & (col_ids < cols)


def kernel(
    groups, chips, wave, ldim, rdim, tout, tin, left_hbm, right_hbm, out,
    blk, left, right, mids, cum, held, prev, last,
    sbuf0, rbuf0, acc1, sbuf1, rbuf1, sbuf2, rbuf2,
    load_sem, zs, zr, ps, pr, xs, xr, s0, r0, s1, r1, s2, r2,
):
    m = lax.axis_index("mpo")
    s = lax.axis_index("sec")
    z, c = s // CORES, s % CORES
    mate = z * CORES + 1 - c
    size = wave.shape[1]
    quarter = size // groups
    tasks = left.shape[0]
    sectors = chips * CORES

    def rows_of(g):
        return pl.ds(pl.multiple_of(g * quarter, quarter), quarter)

    def remote(src, dst, ssem, rsem, dev):
        return pltpu.make_async_remote_copy(
            src_ref=src, dst_ref=dst, send_sem=ssem, recv_sem=rsem,
            device_id=dev, device_id_type=pl.DeviceIdType.MESH,
        )

    loads = [
        pltpu.make_async_copy(left_hbm, left, load_sem.at[0]),
        pltpu.make_async_copy(right_hbm, right, load_sem.at[1]),
    ]
    for copy in loads:
        copy.start()
    barrier = pltpu.get_barrier_semaphore()
    mpo_peers = [lax.rem(m + j, groups) for j in range(1, groups)]
    chip_peers = [lax.rem(z + k, chips) for k in range(1, chips)]
    chip_from = [lax.rem(z + chips - k, chips) for k in range(1, chips)]
    peers = [(m, mate)] + [(g, s) for g in mpo_peers] + [(m, p * CORES + c) for p in chip_peers]
    for dev in peers:
        pl.semaphore_signal(barrier, inc=1, device_id=dev, device_id_type=pl.DeviceIdType.MESH)
    rows, cols = ldim[0], rdim[0]
    blk[s] = jnp.where(live((size, size), 0, rows, cols), wave[0], jnp.zeros_like(wave[0]))
    pl.semaphore_wait(barrier, len(peers))

    sends = []

    def go(copy):
        copy.start()
        sends.append(copy)
        return copy

    z_copies = []
    for k, p in enumerate(chip_peers):
        part = blk.at[s, rows_of(m)]
        z_copies.append(go(remote(part, part, zs.at[k], zr.at[k], (m, p * CORES + c))))
    p_copies = [go(remote(blk.at[s], blk.at[s], ps.at[0], pr.at[0], (m, mate)))]

    def clear(q, _):
        last[q] = 0
        return 0

    lax.fori_loop(0, sectors, clear, 0)

    def link(t, _):
        o = tout[t]

        def look(q, found):
            seen = last[q]
            hit = o == q
            last[q] = jnp.where(hit, t + 1, seen)
            return jnp.where(hit, seen, found)

        prev[t] = lax.fori_loop(0, sectors, look, 0, unroll=8)
        return 0

    lax.fori_loop(0, tasks, link, 0)
    cum[0] = jnp.zeros_like(cum[0])

    x_copies = []
    for k in range(chips - 1):
        z_copies[k].wait_recv()
        part = blk.at[chip_from[k] * CORES + c, rows_of(m)]
        x_copies.append([
            go(remote(part, part, xs.at[k, j], xr.at[k, j], (g, s)))
            for j, g in enumerate(mpo_peers)
        ])
    for k in range(chips - 1):
        for copy in x_copies[k]:
            copy.wait_recv()
        whole = blk.at[chip_from[k] * CORES + c]
        p_copies.append(go(remote(whole, whole, ps.at[k + 1], pr.at[k + 1], (m, mate))))
    for copy in loads:
        copy.wait()
    for copy in p_copies:
        copy.wait_recv()

    def first(i, _):
        for u in range(GROUP):
            t = i * GROUP + u
            mids[t] = jnp.dot(
                left[t], blk[tin[t]], preferred_element_type=jnp.float32
            ).astype(jnp.bfloat16)
        return 0

    lax.fori_loop(0, tasks // GROUP, first, 0)

    def second(i, _):
        for u in range(GROUP):
            t = i * GROUP + u
            product = lax.dot_general(
                mids[t], right[t], (((1,), (1,)), ((), ())), preferred_element_type=jnp.float32
            )
            cum[t + 1] = cum[prev[t]] + product
        return 0

    lax.fori_loop(0, tasks // GROUP, second, 0)

    order = chip_peers + [z]
    r0_copies = []
    for i, p in enumerate(order):
        sbuf0[i] = cum[last[p * CORES + 1 - c]].astype(jnp.bfloat16)
        r0_copies.append(go(remote(sbuf0.at[i], rbuf0.at[i], s0.at[i], r0.at[i], (m, mate))))
    r1_copies = []
    for i, p in enumerate(order):
        r0_copies[i].wait_recv()
        total = cum[last[p * CORES + c]] + rbuf0[i].astype(jnp.float32)
        held[...] = total
        sbuf1[i] = total.astype(jnp.bfloat16)
        r1_copies.append([
            go(remote(sbuf1.at[i, rows_of(g)], rbuf1.at[i, j], s1.at[i, j], r1.at[i, j], (g, s)))
            for j, g in enumerate(mpo_peers)
        ])
        acc1[i] = held[rows_of(m), :]
    r2_copies = []
    for i, p in enumerate(order):
        total = acc1[i]
        for j in range(groups - 1):
            r1_copies[i][j].wait_recv()
            total = total + rbuf1[i, j].astype(jnp.float32)
        if i < chips - 1:
            sbuf2[i] = total.astype(jnp.bfloat16)
            r2_copies.append(
                go(remote(sbuf2.at[i], rbuf2.at[i], s2.at[i], r2.at[i], (m, p * CORES + c)))
            )
    for k in range(chips - 1):
        r2_copies[k].wait_recv()
        total = total + rbuf2[k].astype(jnp.float32)
    keep = live(total.shape, m * quarter, rows, cols)
    out[0] = jnp.where(keep, total, jnp.zeros_like(total)).astype(jnp.bfloat16)
    for copy in sends:
        copy.wait_send()


def on_device(
    wavefunction, left_dims, right_dims, left_environment_block, right_env, task_out, task_in
):
    groups, sec = lax.axis_size("mpo"), lax.axis_size("sec")
    chips = sec // CORES
    _, size, width = wavefunction.shape
    quarter = size // groups
    tasks = task_out.shape[0]
    bf16, f32 = jnp.bfloat16, jnp.float32
    smem = pl.BlockSpec(memory_space=pltpu.SMEM)
    vmem = pl.BlockSpec(memory_space=pltpu.VMEM)
    dma = pltpu.SemaphoreType.DMA
    near, far = max(groups - 1, 1), max(chips - 1, 1)
    return pl.pallas_call(
        functools.partial(kernel, groups, chips),
        out_shape=jax.ShapeDtypeStruct((1, quarter, width), bf16),
        in_specs=[vmem, smem, smem, smem, smem]
        + [pl.BlockSpec(memory_space=pl.ANY)] * 2,
        out_specs=vmem,
        scratch_shapes=[
            pltpu.VMEM((sec, size, width), bf16),
            pltpu.VMEM((tasks, size, size), bf16),
            pltpu.VMEM((tasks, size, size), bf16),
            pltpu.VMEM((tasks, size, width), bf16),
            pltpu.VMEM((tasks + 1, size, width), f32),
            pltpu.VMEM((size, width), f32),
            pltpu.SMEM((tasks,), jnp.int32),
            pltpu.SMEM((sec,), jnp.int32),
            pltpu.VMEM((chips, size, width), bf16),
            pltpu.VMEM((chips, size, width), bf16),
            pltpu.VMEM((chips, quarter, width), f32),
            pltpu.VMEM((chips, size, width), bf16),
            pltpu.VMEM((chips, near, quarter, width), bf16),
            pltpu.VMEM((far, quarter, width), bf16),
            pltpu.VMEM((far, quarter, width), bf16),
            dma((2,)),
            dma((far,)), dma((far,)),
            dma((chips,)), dma((chips,)),
            dma((far, near)), dma((far, near)),
            dma((chips,)), dma((chips,)),
            dma((chips, near)), dma((chips, near)),
            dma((far,)), dma((far,)),
        ],
        compiler_params=pltpu.CompilerParams(
            collective_id=0, has_side_effects=True, vmem_limit_bytes=60 * 1024 * 1024
        ),
        name="apply_blocks",
    )(wavefunction, left_dims, right_dims, task_out, task_in, left_environment_block, right_env)


def solution(mesh):
    return jax.shard_map(
        on_device,
        mesh=mesh,
        in_specs=(
            P("sec", None, None),
            P("sec"),
            P("sec"),
            P(("mpo", "sec"), None, None),
            P(("mpo", "sec"), None, None),
            P(("mpo", "sec")),
            P(("mpo", "sec")),
        ),
        out_specs=P("sec", "mpo", None),
        check_vma=False,
    )
```

```python
import functools

import jax
import jax.numpy as jnp
from jax import lax
from jax.experimental import pallas as pl
from jax.experimental.pallas import tpu as pltpu
from jax.sharding import PartitionSpec as P

CORES = 2
GROUP = 20


def live(shape, row0, rows, cols):
    row_ids = lax.broadcasted_iota(jnp.int32, shape, 0) + row0
    col_ids = lax.broadcasted_iota(jnp.int32, shape, 1)
    return (row_ids < rows) & (col_ids < cols)


def kernel(
    groups, chips, wave, ldim_hbm, rdim_hbm, tout, tin, left_hbm, right_hbm, out,
    blk, left, right, mids, cum, held, prev, last, ldim, rdim,
    sbuf0, rbuf0, acc1, sbuf1, rbuf1, sbuf2, rbuf2,
    load_sem, zs, zr, ps, pr, xs, xr, s0, r0, s1, r1, s2, r2,
):
    m = lax.axis_index("mpo")
    s = lax.axis_index("sec")
    z, c = s // CORES, s % CORES
    mate = z * CORES + 1 - c
    size = wave.shape[1]
    quarter = size // groups
    tasks = left.shape[0]
    sectors = chips * CORES

    def rows_of(g):
        return pl.ds(pl.multiple_of(g * quarter, quarter), quarter)

    def remote(src, dst, ssem, rsem, dev):
        return pltpu.make_async_remote_copy(
            src_ref=src, dst_ref=dst, send_sem=ssem, recv_sem=rsem,
            device_id=dev, device_id_type=pl.DeviceIdType.MESH,
        )

    loads = [
        pltpu.make_async_copy(left_hbm, left, load_sem.at[0]),
        pltpu.make_async_copy(right_hbm, right, load_sem.at[1]),
    ]
    dims = [
        pltpu.make_async_copy(ldim_hbm, ldim, load_sem.at[2]),
        pltpu.make_async_copy(rdim_hbm, rdim, load_sem.at[3]),
    ]
    for copy in dims + loads:
        copy.start()
    barrier = pltpu.get_barrier_semaphore()
    mpo_peers = [lax.rem(m + j, groups) for j in range(1, groups)]
    chip_peers = [lax.rem(z + k, chips) for k in range(1, chips)]
    chip_from = [lax.rem(z + chips - k, chips) for k in range(1, chips)]
    peers = [(m, mate)] + [(g, s) for g in mpo_peers] + [(m, p * CORES + c) for p in chip_peers]
    for dev in peers:
        pl.semaphore_signal(barrier, inc=1, device_id=dev, device_id_type=pl.DeviceIdType.MESH)
    for copy in dims:
        copy.wait()
    rows, cols = ldim[0], rdim[0]
    blk[s] = jnp.where(live((size, size), 0, rows, cols), wave[0], jnp.zeros_like(wave[0]))
    pl.semaphore_wait(barrier, len(peers))

    sends = []

    def go(copy):
        copy.start()
        sends.append(copy)
        return copy

    z_copies = []
    for k, p in enumerate(chip_peers):
        part = blk.at[s, rows_of(m)]
        z_copies.append(go(remote(part, part, zs.at[k], zr.at[k], (m, p * CORES + c))))
    p_copies = [go(remote(blk.at[s], blk.at[s], ps.at[0], pr.at[0], (m, mate)))]

    def clear(q, _):
        last[q] = 0
        return 0

    lax.fori_loop(0, sectors, clear, 0)

    def link(t, _):
        o = tout[t]

        def look(q, found):
            seen = last[q]
            hit = o == q
            last[q] = jnp.where(hit, t + 1, seen)
            return jnp.where(hit, seen, found)

        prev[t] = lax.fori_loop(0, sectors, look, 0, unroll=8)
        return 0

    lax.fori_loop(0, tasks, link, 0)
    cum[0] = jnp.zeros_like(cum[0])

    x_copies = []
    for k in range(chips - 1):
        z_copies[k].wait_recv()
        part = blk.at[chip_from[k] * CORES + c, rows_of(m)]
        x_copies.append([
            go(remote(part, part, xs.at[k, j], xr.at[k, j], (g, s)))
            for j, g in enumerate(mpo_peers)
        ])
    for k in range(chips - 1):
        for copy in x_copies[k]:
            copy.wait_recv()
        whole = blk.at[chip_from[k] * CORES + c]
        p_copies.append(go(remote(whole, whole, ps.at[k + 1], pr.at[k + 1], (m, mate))))
    for copy in loads:
        copy.wait()
    for copy in p_copies:
        copy.wait_recv()

    def first(i, _):
        for u in range(GROUP):
            t = i * GROUP + u
            mids[t] = jnp.dot(
                left[t], blk[tin[t]], preferred_element_type=jnp.float32
            ).astype(jnp.bfloat16)
        return 0

    lax.fori_loop(0, tasks // GROUP, first, 0)

    def second(i, _):
        for u in range(GROUP):
            t = i * GROUP + u
            product = lax.dot_general(
                mids[t], right[t], (((1,), (1,)), ((), ())), preferred_element_type=jnp.float32
            )
            cum[t + 1] = cum[prev[t]] + product
        return 0

    lax.fori_loop(0, tasks // GROUP, second, 0)

    order = chip_peers + [z]
    r0_copies = []
    for i, p in enumerate(order):
        sbuf0[i] = cum[last[p * CORES + 1 - c]].astype(jnp.bfloat16)
        r0_copies.append(go(remote(sbuf0.at[i], rbuf0.at[i], s0.at[i], r0.at[i], (m, mate))))
    r1_copies = []
    for i, p in enumerate(order):
        r0_copies[i].wait_recv()
        total = cum[last[p * CORES + c]] + rbuf0[i].astype(jnp.float32)
        held[...] = total
        sbuf1[i] = total.astype(jnp.bfloat16)
        r1_copies.append([
            go(remote(sbuf1.at[i, rows_of(g)], rbuf1.at[i, j], s1.at[i, j], r1.at[i, j], (g, s)))
            for j, g in enumerate(mpo_peers)
        ])
        acc1[i] = held[rows_of(m), :]
    r2_copies = []
    for i, p in enumerate(order):
        total = acc1[i]
        for j in range(groups - 1):
            r1_copies[i][j].wait_recv()
            total = total + rbuf1[i, j].astype(jnp.float32)
        if i < chips - 1:
            sbuf2[i] = total.astype(jnp.bfloat16)
            r2_copies.append(
                go(remote(sbuf2.at[i], rbuf2.at[i], s2.at[i], r2.at[i], (m, p * CORES + c)))
            )
    for k in range(chips - 1):
        r2_copies[k].wait_recv()
        total = total + rbuf2[k].astype(jnp.float32)
    keep = live(total.shape, m * quarter, rows, cols)
    out[0] = jnp.where(keep, total, jnp.zeros_like(total)).astype(jnp.bfloat16)
    for copy in sends:
        copy.wait_send()


def on_device(
    wavefunction, left_dims, right_dims, left_environment_block, right_env, task_out, task_in
):
    groups, sec = lax.axis_size("mpo"), lax.axis_size("sec")
    chips = sec // CORES
    _, size, width = wavefunction.shape
    quarter = size // groups
    tasks = task_out.shape[0]
    bf16, f32 = jnp.bfloat16, jnp.float32
    smem = pl.BlockSpec(memory_space=pltpu.SMEM)
    hbm = pl.BlockSpec(memory_space=pl.ANY)
    vmem = pl.BlockSpec(memory_space=pltpu.VMEM)
    dma = pltpu.SemaphoreType.DMA
    near, far = max(groups - 1, 1), max(chips - 1, 1)
    return pl.pallas_call(
        functools.partial(kernel, groups, chips),
        out_shape=jax.ShapeDtypeStruct((1, quarter, width), bf16),
        in_specs=[vmem, hbm, hbm, smem, smem, hbm, hbm],
        out_specs=vmem,
        scratch_shapes=[
            pltpu.VMEM((sec, size, width), bf16),
            pltpu.VMEM((tasks, size, size), bf16),
            pltpu.VMEM((tasks, size, size), bf16),
            pltpu.VMEM((tasks, size, width), bf16),
            pltpu.VMEM((tasks + 1, size, width), f32),
            pltpu.VMEM((size, width), f32),
            pltpu.SMEM((tasks,), jnp.int32),
            pltpu.SMEM((sec,), jnp.int32),
            pltpu.SMEM((1,), jnp.int32),
            pltpu.SMEM((1,), jnp.int32),
            pltpu.VMEM((chips, size, width), bf16),
            pltpu.VMEM((chips, size, width), bf16),
            pltpu.VMEM((chips, quarter, width), f32),
            pltpu.VMEM((chips, size, width), bf16),
            pltpu.VMEM((chips, near, quarter, width), bf16),
            pltpu.VMEM((far, quarter, width), bf16),
            pltpu.VMEM((far, quarter, width), bf16),
            dma((4,)),
            dma((far,)), dma((far,)),
            dma((chips,)), dma((chips,)),
            dma((far, near)), dma((far, near)),
            dma((chips,)), dma((chips,)),
            dma((chips, near)), dma((chips, near)),
            dma((far,)), dma((far,)),
        ],
        compiler_params=pltpu.CompilerParams(
            collective_id=0, has_side_effects=True, vmem_limit_bytes=60 * 1024 * 1024
        ),
        name="apply_blocks",
    )(wavefunction, left_dims, right_dims, task_out, task_in, left_environment_block, right_env)


def solution(mesh):
    return jax.shard_map(
        on_device,
        mesh=mesh,
        in_specs=(
            P("sec", None, None),
            P("sec"),
            P("sec"),
            P(("mpo", "sec"), None, None),
            P(("mpo", "sec"), None, None),
            P(("mpo", "sec")),
            P(("mpo", "sec")),
        ),
        out_specs=P("sec", "mpo", None),
        check_vma=False,
    )
```

```python
import functools

import jax
import jax.numpy as jnp
from jax import lax
from jax.experimental import pallas as pl
from jax.experimental.pallas import tpu as pltpu
from jax.sharding import PartitionSpec as P

CORES = 2
GROUP = 20


def live(shape, row0, rows, cols):
    row_ids = lax.broadcasted_iota(jnp.int32, shape, 0) + row0
    col_ids = lax.broadcasted_iota(jnp.int32, shape, 1)
    return (row_ids < rows) & (col_ids < cols)


def kernel(
    groups, chips, wave, ldim_hbm, rdim_hbm, tout, tin, left_hbm, right_hbm, out,
    blk, left, right, mids, cum, held, prev, last, ldim, rdim,
    sbuf0, rbuf0, acc1, sbuf1, rbuf1, sbuf2, rbuf2,
    load_sem, zs, zr, ps, pr, xs, xr, s0, r0, s1, r1, s2, r2,
):
    m = lax.axis_index("mpo")
    s = lax.axis_index("sec")
    z, c = s // CORES, s % CORES
    mate = z * CORES + 1 - c
    size = wave.shape[1]
    quarter = size // groups
    tasks = left.shape[0]
    sectors = chips * CORES

    def rows_of(g):
        return pl.ds(pl.multiple_of(g * quarter, quarter), quarter)

    def remote(src, dst, ssem, rsem, dev):
        return pltpu.make_async_remote_copy(
            src_ref=src, dst_ref=dst, send_sem=ssem, recv_sem=rsem,
            device_id=dev, device_id_type=pl.DeviceIdType.MESH,
        )

    loads = [
        pltpu.make_async_copy(left_hbm, left, load_sem.at[0]),
        pltpu.make_async_copy(right_hbm, right, load_sem.at[1]),
    ]
    dims = [
        pltpu.make_async_copy(ldim_hbm, ldim, load_sem.at[2]),
        pltpu.make_async_copy(rdim_hbm, rdim, load_sem.at[3]),
    ]
    for copy in dims + loads:
        copy.start()
    barrier = pltpu.get_barrier_semaphore()
    mpo_peers = [lax.rem(m + j, groups) for j in range(1, groups)]
    chip_peers = [lax.rem(z + k, chips) for k in range(1, chips)]
    chip_from = [lax.rem(z + chips - k, chips) for k in range(1, chips)]
    peers = [(m, mate)] + [(g, s) for g in mpo_peers] + [(m, p * CORES + c) for p in chip_peers]
    for dev in peers:
        pl.semaphore_signal(barrier, inc=1, device_id=dev, device_id_type=pl.DeviceIdType.MESH)
    for copy in dims:
        copy.wait()
    rows, cols = ldim[0], rdim[0]
    blk[s] = jnp.where(live((size, size), 0, rows, cols), wave[0], jnp.zeros_like(wave[0]))
    pl.semaphore_wait(barrier, len(peers))

    sends = []

    def go(copy):
        copy.start()
        sends.append(copy)
        return copy

    z_copies = []
    for k, p in enumerate(chip_peers):
        part = blk.at[s, rows_of(m)]
        z_copies.append(go(remote(part, part, zs.at[k], zr.at[k], (m, p * CORES + c))))
    p_copies = [go(remote(blk.at[s], blk.at[s], ps.at[0], pr.at[0], (m, mate)))]

    def clear(q, _):
        last[q] = 0
        return 0

    lax.fori_loop(0, sectors, clear, 0)

    def link(t, _):
        o = tout[t]

        def look(q, found):
            seen = last[q]
            hit = o == q
            last[q] = jnp.where(hit, t + 1, seen)
            return jnp.where(hit, seen, found)

        prev[t] = lax.fori_loop(0, sectors, look, 0, unroll=8)
        return 0

    lax.fori_loop(0, tasks, link, 0)
    cum[0] = jnp.zeros_like(cum[0])

    x_copies = []
    for k in range(chips - 1):
        z_copies[k].wait_recv()
        part = blk.at[chip_from[k] * CORES + c, rows_of(m)]
        x_copies.append([
            go(remote(part, part, xs.at[k, j], xr.at[k, j], (g, s)))
            for j, g in enumerate(mpo_peers)
        ])
    for k in range(chips - 1):
        for copy in x_copies[k]:
            copy.wait_recv()
        whole = blk.at[chip_from[k] * CORES + c]
        p_copies.append(go(remote(whole, whole, ps.at[k + 1], pr.at[k + 1], (m, mate))))
    for copy in loads:
        copy.wait()
    for copy in p_copies:
        copy.wait_recv()

    def multiply(i, _):
        group = [i * GROUP + u for u in range(GROUP)]
        for t in group:
            mids[t] = jnp.dot(
                left[t], blk[tin[t]], preferred_element_type=jnp.float32
            ).astype(jnp.bfloat16)
        for t in group:
            product = lax.dot_general(
                mids[t], right[t], (((1,), (1,)), ((), ())), preferred_element_type=jnp.float32
            )
            cum[t + 1] = cum[prev[t]] + product
        return 0

    lax.fori_loop(0, tasks // GROUP, multiply, 0)

    order = chip_peers + [z]
    r0_copies = []
    for i, p in enumerate(order):
        sbuf0[i] = cum[last[p * CORES + 1 - c]].astype(jnp.bfloat16)
        r0_copies.append(go(remote(sbuf0.at[i], rbuf0.at[i], s0.at[i], r0.at[i], (m, mate))))
    r1_copies = []
    for i, p in enumerate(order):
        r0_copies[i].wait_recv()
        total = cum[last[p * CORES + c]] + rbuf0[i].astype(jnp.float32)
        held[...] = total
        sbuf1[i] = total.astype(jnp.bfloat16)
        r1_copies.append([
            go(remote(sbuf1.at[i, rows_of(g)], rbuf1.at[i, j], s1.at[i, j], r1.at[i, j], (g, s)))
            for j, g in enumerate(mpo_peers)
        ])
        acc1[i] = held[rows_of(m), :]
    r2_copies = []
    for i, p in enumerate(order):
        total = acc1[i]
        for j in range(groups - 1):
            r1_copies[i][j].wait_recv()
            total = total + rbuf1[i, j].astype(jnp.float32)
        if i < chips - 1:
            sbuf2[i] = total.astype(jnp.bfloat16)
            r2_copies.append(
                go(remote(sbuf2.at[i], rbuf2.at[i], s2.at[i], r2.at[i], (m, p * CORES + c)))
            )
    for k in range(chips - 1):
        r2_copies[k].wait_recv()
        total = total + rbuf2[k].astype(jnp.float32)
    keep = live(total.shape, m * quarter, rows, cols)
    out[0] = jnp.where(keep, total, jnp.zeros_like(total)).astype(jnp.bfloat16)
    for copy in sends:
        copy.wait_send()


def on_device(
    wavefunction, left_dims, right_dims, left_environment_block, right_env, task_out, task_in
):
    groups, sec = lax.axis_size("mpo"), lax.axis_size("sec")
    chips = sec // CORES
    _, size, width = wavefunction.shape
    quarter = size // groups
    tasks = task_out.shape[0]
    bf16, f32 = jnp.bfloat16, jnp.float32
    smem = pl.BlockSpec(memory_space=pltpu.SMEM)
    hbm = pl.BlockSpec(memory_space=pl.ANY)
    vmem = pl.BlockSpec(memory_space=pltpu.VMEM)
    dma = pltpu.SemaphoreType.DMA
    near, far = max(groups - 1, 1), max(chips - 1, 1)
    return pl.pallas_call(
        functools.partial(kernel, groups, chips),
        out_shape=jax.ShapeDtypeStruct((1, quarter, width), bf16),
        in_specs=[vmem, hbm, hbm, smem, smem, hbm, hbm],
        out_specs=vmem,
        scratch_shapes=[
            pltpu.VMEM((sec, size, width), bf16),
            pltpu.VMEM((tasks, size, size), bf16),
            pltpu.VMEM((tasks, size, size), bf16),
            pltpu.VMEM((tasks, size, width), bf16),
            pltpu.VMEM((tasks + 1, size, width), f32),
            pltpu.VMEM((size, width), f32),
            pltpu.SMEM((tasks,), jnp.int32),
            pltpu.SMEM((sec,), jnp.int32),
            pltpu.SMEM((1,), jnp.int32),
            pltpu.SMEM((1,), jnp.int32),
            pltpu.VMEM((chips, size, width), bf16),
            pltpu.VMEM((chips, size, width), bf16),
            pltpu.VMEM((chips, quarter, width), f32),
            pltpu.VMEM((chips, size, width), bf16),
            pltpu.VMEM((chips, near, quarter, width), bf16),
            pltpu.VMEM((far, quarter, width), bf16),
            pltpu.VMEM((far, quarter, width), bf16),
            dma((4,)),
            dma((far,)), dma((far,)),
            dma((chips,)), dma((chips,)),
            dma((far, near)), dma((far, near)),
            dma((chips,)), dma((chips,)),
            dma((chips, near)), dma((chips, near)),
            dma((far,)), dma((far,)),
        ],
        compiler_params=pltpu.CompilerParams(
            collective_id=0, has_side_effects=True, vmem_limit_bytes=60 * 1024 * 1024
        ),
        name="apply_blocks",
    )(wavefunction, left_dims, right_dims, task_out, task_in, left_environment_block, right_env)


def solution(mesh):
    return jax.shard_map(
        on_device,
        mesh=mesh,
        in_specs=(
            P("sec", None, None),
            P("sec"),
            P("sec"),
            P(("mpo", "sec"), None, None),
            P(("mpo", "sec"), None, None),
            P(("mpo", "sec")),
            P(("mpo", "sec")),
        ),
        out_specs=P("sec", "mpo", None),
        check_vma=False,
    )
```
